32 devices in a mesh: row: 8 (over y, x, core), col: 4 (over z).
Axes of the slice: x: 2, y: 2, z: 4, core: 2. Of those that a mesh axis runs over, the one named last changes fastest.
Arguments:
- tokens: bfloat16 [1024, 8192], P('row', 'col'), may hold values from -200 to 200
- norm_gain: float32 [8192], P('col'), may hold values from 0.1 to 1.9
- gate_weight: bfloat16 [8192, 28672], P('col', 'row'), may hold values from -0.0625 to 0.0625
- up_weight: bfloat16 [8192, 28672], P('col', 'row'), may hold values from -0.0625 to 0.0625
- down_weight: bfloat16 [28672, 8192], P('row', 'col'), may hold values from -0.03125 to 0.03125
Outputs:
- mixed: bfloat16 [1024, 8192], P('row', 'col')
The draws below stay inside these ranges and needn't reach their ends.
All inputs are finite; a program needn't handle non-finite values.
Results may differ from the reference program's by a relative error of at most 0.028.
Values may be sent and summed in bfloat16 or wider, within the bound.
A program may use at most 128 MiB of HBM per device.

```python
import math
import jax
import jax.numpy as jnp
from jax import lax

D = 8192
FF = 28672
TOKENS = 1024
N_ROW = 8
N_COL = 4


def draw_tokens(key, part):
    first, second, third = jax.random.split(jax.random.fold_in(key, 11), 3)
    ramp = jnp.sqrt(1.0 + 2.0 * jnp.arange(D, dtype=jnp.float32) / max(D - 1, 1))
    rough = jnp.exp(jax.random.uniform(second, (D,), jnp.float32, -0.35, 0.35))
    column_scale = ramp * rough
    base = jax.random.normal(first, (TOKENS, D), jnp.float32)
    row_scale = jnp.exp(jax.random.uniform(third, (TOKENS, 1), jnp.float32, 0.0, math.log(10.0)))
    values = jnp.clip(base * column_scale[None, :] * row_scale, -200.0, 200.0)
    return values.astype(jnp.bfloat16)


def level_of(rng, extent, shards, least, largest):
    factor_of = 1.0
    for axis_at, blocks in shards:
        heights = jax.random.uniform(jax.random.fold_in(jax.random.fold_in(rng, 6), axis_at), (blocks,), jnp.float32, least / len(shards), largest / len(shards))
        factor_of = factor_of * jnp.repeat(jnp.exp(heights), extent[axis_at] // blocks).reshape((-1,) + (1,) * (len(extent) - 1 - axis_at))
    return factor_of


def gaussian(stream_key, extent, width, most, cuts=(), kind=jnp.bfloat16):
    level = level_of(stream_key, extent, cuts, -0.22, 0.18) if cuts else 1.0
    array = jax.random.normal(stream_key, extent, jnp.float32) * width * level
    return jnp.minimum(jnp.maximum(array, -most), most).astype(kind)


def setup_inputs(seed: int = 0) -> dict:
    streams_of = jax.random.split(jax.random.key(seed), 6)
    tokens = draw_tokens(jax.random.fold_in(streams_of[5], 71), 0)
    norm_gain = jnp.clip(1.0 + 0.18 * jax.random.normal(streams_of[1], (D,), jnp.float32), 0.1, 1.9)
    gate_weight = gaussian(streams_of[2], (D, FF), D ** -0.5, 0.0625, ((0, 4), (1, 8)))
    up_weight = gaussian(streams_of[3], (D, FF), D ** -0.5, 0.0625, ((0, 4), (1, 8)))
    down_weight = gaussian(streams_of[4], (FF, D), FF ** -0.5, 0.03125, ((0, 8), (1, 4)))
    return {"tokens": tokens, "norm_gain": norm_gain, "gate_weight": gate_weight, "up_weight": up_weight, "down_weight": down_weight}


def reference(tokens, norm_gain, gate_weight, up_weight, down_weight):
    values = tokens.astype(jnp.float32)
    squares = lax.optimization_barrier(jnp.sum(values * values, axis=1))
    scale = lax.rsqrt(squares / D + 1e-05)
    normed = (values * scale[:, None] * norm_gain[None, :]).astype(jnp.bfloat16)
    group = D // N_COL
    gate = jnp.zeros((TOKENS, FF), jnp.float32)
    up = jnp.zeros((TOKENS, FF), jnp.float32)
    for index in range(N_COL):
        rows = normed[:, index * group:(index + 1) * group]
        part_gate = jnp.dot(rows, gate_weight[index * group:(index + 1) * group], preferred_element_type=jnp.float32)
        part_up = jnp.dot(rows, up_weight[index * group:(index + 1) * group], preferred_element_type=jnp.float32)
        gate = gate + part_gate.astype(jnp.bfloat16).astype(jnp.float32)
        up = up + part_up.astype(jnp.bfloat16).astype(jnp.float32)
    hidden = (jax.nn.silu(gate) * up).astype(jnp.bfloat16)
    hgroup = FF // N_ROW
    mixed = jnp.zeros((TOKENS, D), jnp.float32)
    for index in range(N_ROW):
        part = jnp.dot(hidden[:, index * hgroup:(index + 1) * hgroup], down_weight[index * hgroup:(index + 1) * hgroup], preferred_element_type=jnp.float32)
        mixed = mixed + part.astype(jnp.bfloat16).astype(jnp.float32)
    return mixed.astype(jnp.bfloat16)
```

```python
import functools

import jax
import jax.numpy as jnp
from jax import lax
from jax.experimental import pallas as pl
from jax.experimental.pallas import tpu as pltpu
from jax.sharding import PartitionSpec as P

MESH = pl.DeviceIdType.MESH
LAG_SUM = 2
LAG_HID = 1
STAGES = 4
KEEP = 2
PIECES = 4


def exclusive_or(a, b, bits):
    total = a + b
    for bit in range(bits):
        size = 1 << bit
        total = total - 2 * size * (((a // size) % 2) * ((b // size) % 2))
    return total


def kernel(
    plan, tok, gain, gate_w, up_w, down_w, out,
    xall, wgu, wd, gu_in, gu_out, ybuf, hid, acc, own, rs_in, rs_out,
    sq_out, sq_in, tot_out, tot_in, scale,
    own_sem, wg_sem, wu_sem, wd_sem, ag_send, ag_recv, rs_send, rs_recv,
    sq_send, sq_recv, tot_send, tot_recv, gs_send, gs_recv, hs_send, hs_recv,
):
    rows, cols, part, depth, width, chunks = plan
    hops = cols - 1
    units = rows * chunks
    half = chunks * width
    lag = hops * (LAG_SUM + LAG_HID)
    slots = gu_in.shape[1]
    places = hid.shape[1]
    banks = acc.shape[0]
    bits = rows.bit_length() - 1
    r, p = lax.axis_index("row"), lax.axis_index("col")
    spot = (p, hops - p)
    after = (p + 1, p - 1)
    before = (p - 1, p + 1)
    near = jnp.minimum(spot[0], spot[1])
    far = hops - near

    def mask(i):
        if isinstance(i, int):
            return 0 if i == 0 else (1 if i == rows - 1 else i + 1)
        return jnp.where(i == 0, 0, jnp.where(i == rows - 1, 1, i + 1))

    def partner(i):
        return exclusive_or(r, mask(i), bits)

    def weight_copies(s, j):
        at = s * half + j * width
        c = s * chunks + j
        return (
            pltpu.make_async_copy(gate_w.at[:, pl.ds(at, width)], wgu.at[c, :, pl.ds(0, width)], wg_sem.at[c]),
            pltpu.make_async_copy(up_w.at[:, pl.ds(at, width)], wgu.at[c, :, pl.ds(width, width)], wu_sem.at[c]),
        )

    def down_copy(s, j):
        c = s * chunks + j
        return pltpu.make_async_copy(down_w.at[pl.ds(s * half + j * width, width)], wd.at[c], wd_sem.at[c])

    own_copy = pltpu.make_async_copy(tok, xall.at[0], own_sem)
    own_copy.start()
    for s in (0, 1):
        for one in weight_copies(s, 0):
            one.start()

    barrier = pltpu.get_barrier_semaphore()
    for i in range(1, rows):
        pl.semaphore_signal(barrier, inc=1, device_id=(partner(i), p), device_id_type=MESH)
    for d in range(1, cols):
        pl.semaphore_signal(barrier, inc=1, device_id=(r, (p + d) % cols), device_id_type=MESH)
    pl.semaphore_wait(barrier, rows + cols - 2)

    def spread(i):
        return pltpu.make_async_remote_copy(
            src_ref=tok, dst_ref=xall.at[i], send_sem=ag_send.at[i], recv_sem=ag_recv.at[i],
            device_id=(partner(i), p), device_id_type=MESH)

    for i in range(1, rows):
        spread(i).start()
    for j in range(1, chunks):
        for s in (0, 1):
            for one in weight_copies(s, j):
                one.start()
    for j in range(chunks):
        for s in (0, 1):
            down_copy(s, j).start()

    def square_copy(d):
        return pltpu.make_async_remote_copy(
            src_ref=sq_out, dst_ref=sq_in.at[d], send_sem=sq_send.at[d], recv_sem=sq_recv.at[d],
            device_id=(r, (p + d) % cols), device_id_type=MESH)

    def total_copy(i):
        return pltpu.make_async_remote_copy(
            src_ref=tot_out, dst_ref=tot_in.at[i], send_sem=tot_send.at[i], recv_sem=tot_recv.at[i],
            device_id=(partner(i), p), device_id_type=MESH)

    own_copy.wait()
    squares = jnp.zeros((part, 128), jnp.float32)
    for c in range(depth // 128):
        at = pl.ds(c * 128, 128)
        value = xall[0, :, at].astype(jnp.float32)
        squares = squares + value * value
        xall[0, :, at] = (value * gain[:, at]).astype(jnp.bfloat16)
    sq_out[...] = jnp.broadcast_to(jnp.sum(squares.T, axis=0, keepdims=True), (8, part))
    for d in range(1, cols):
        square_copy(d).start()

    def put_scale(i, total):
        tall = jnp.broadcast_to(total[0:1, :], (128, part)).T
        scale[i] = lax.rsqrt(tall / (depth * cols) + 1e-05)

    def total_squares():
        total = sq_out[...]
        for d in range(1, cols):
            square_copy(d).wait_recv()
            total = total + sq_in[d]
        tot_out[...] = total
        put_scale(0, total)
        for i in range(1, rows):
            total_copy(i).start()

    def sum_copy(s, n):
        stage, slot = lax.rem(n, STAGES), lax.rem(n, slots)
        return pltpu.make_async_remote_copy(
            src_ref=gu_out.at[s, stage], dst_ref=gu_in.at[s, slot],
            send_sem=gs_send.at[s, stage], recv_sem=gs_recv.at[s, slot],
            device_id=(r, after[s]), device_id_type=MESH)

    def hidden_copy(s, m):
        place = lax.rem(m, places)
        return pltpu.make_async_remote_copy(
            src_ref=hid.at[s, place], dst_ref=hid.at[s, place],
            send_sem=hs_send.at[s, place], recv_sem=hs_recv.at[s, place],
            device_id=(r, before[s]), device_id_type=MESH)

    def result_copy(i):
        return pltpu.make_async_remote_copy(
            src_ref=rs_out, dst_ref=rs_in.at[i], send_sem=rs_send, recv_sem=rs_recv.at[i],
            device_id=(partner(i), p), device_id_type=MESH)

    def sums(s, t):
        q = spot[s]
        n = t - LAG_SUM * q
        valid = (n >= 0) & (n < units)

        @pl.when(valid)
        def _():
            i = n // chunks
            j = n - i * chunks

            @pl.when(i == 0)
            def _():
                for one in weight_copies(s, j):
                    one.wait()

            ybuf[...] = jnp.dot(xall[i], wgu[s * chunks + j], preferred_element_type=jnp.float32)

            @pl.when(q > 0)
            def _():
                sum_copy(s, n).wait_recv()
                ybuf[...] += gu_in[s, lax.rem(n, slots)].astype(jnp.float32)

        @pl.when((q < hops) & (n >= STAGES) & (n < units + STAGES))
        def _():
            sum_copy(s, n - STAGES).wait_send()

        @pl.when(valid & (q < hops))
        def _():
            gu_out[s, lax.rem(n, STAGES)] = ybuf[...].astype(jnp.bfloat16)
            sum_copy(s, n).start()

        @pl.when(valid & (q == hops))
        def _():
            factor = scale[n // chunks]
            for c in range(width // 128):
                g = ybuf[:, pl.ds(c * 128, 128)] * factor
                u = ybuf[:, pl.ds(width + c * 128, 128)] * factor
                hid[s, lax.rem(n, places), :, pl.ds(c * 128, 128)] = (jax.nn.silu(g) * u).astype(jnp.bfloat16)
            hidden_copy(s, n).start()

    def hiddens(s, t):
        q = spot[s]
        m = t - lag + LAG_HID * q
        valid = (m >= 0) & (m < units)
        place = lax.rem(jnp.maximum(m, 0), places)

        @pl.when(valid & (q < hops))
        def _():
            hidden_copy(s, m).wait_recv()

        @pl.when(valid & (q < hops) & (q > 0))
        def _():
            hidden_copy(s, m).start()

        @pl.when(valid)
        def _():
            i = m // chunks
            j = m - i * chunks
            bank = lax.rem(i, banks)

            @pl.when(i == 0)
            def _():
                down_copy(s, j).wait()

            leads = (q == far) if s == 0 else ((q == far) & (spot[0] != far))
            fresh = leads & (j == 0)
            wide = depth // PIECES
            for c in range(PIECES):
                at = pl.ds(c * wide, wide)
                value = jnp.dot(hid[s, place], wd[s * chunks + j, :, at], preferred_element_type=jnp.float32)

                @pl.when(fresh)
                def _():
                    acc[bank, :, at] = value

                @pl.when(jnp.logical_not(fresh))
                def _():
                    acc[bank, :, at] += value

        @pl.when((q > 0) & (m >= KEEP) & (m < units + KEEP))
        def _():
            hidden_copy(s, m - KEEP).wait_send()

    def step(t, carry):
        first = t - LAG_SUM * near

        @pl.when((first >= chunks) & (first < units) & (first % chunks == 0))
        def _():
            i = first // chunks
            spread(i).wait_recv()
            total_copy(i).wait_recv()
            for c in range(depth // 128):
                at = pl.ds(c * 128, 128)
                xall[i, :, at] = (xall[i, :, at].astype(jnp.float32) * gain[:, at]).astype(jnp.bfloat16)
            put_scale(i, tot_in[i])

        sums(0, t)
        sums(1, t)

        @pl.when(first == 1)
        def _():
            total_squares()

        hiddens(0, t)
        hiddens(1, t)

        last = t - lag + LAG_HID * near

        @pl.when((last >= 0) & (last < units) & (last % chunks == chunks - 1))
        def _():
            i = last // chunks
            bank = lax.rem(i, banks)

            @pl.when(i == 0)
            def _():
                own[...] = acc[bank]

            @pl.when(i >= 2)
            def _():
                result_copy(i - 1).wait_send()

            @pl.when(i > 0)
            def _():
                rs_out[...] = acc[bank].astype(jnp.bfloat16)
                result_copy(i).start()

            @pl.when(i >= 2)
            def _():
                result_copy(i - 1).wait_recv()
                own[...] += rs_in[i - 1].astype(jnp.float32)

        return carry

    lax.fori_loop(0, units + lag + KEEP, step, 0)

    if rows > 1:
        result_copy(rows - 1).wait_send()
        result_copy(rows - 1).wait_recv()
        out[...] = (own[...] + rs_in[rows - 1].astype(jnp.float32)).astype(jnp.bfloat16)
    else:
        out[...] = own[...].astype(jnp.bfloat16)
    for i in range(1, rows):
        spread(i).wait_send()
        total_copy(i).wait_send()
    for d in range(1, cols):
        square_copy(d).wait_send()


def make_body(rows, cols):
    hops = cols - 1
    assert rows & (rows - 1) == 0 and cols > 1

    def body(tokens, norm_gain, gate_weight, up_weight, down_weight):
        part, depth = tokens.shape
        wide = gate_weight.shape[1]
        width = 256 if wide % 512 == 0 else 128
        chunks = wide // (2 * width)
        assert part == 128 and wide % (2 * width) == 0
        lag = hops * (LAG_SUM + LAG_HID)
        slots, places = lag + 2, lag + 2 + KEEP
        banks = -(-LAG_HID * hops // chunks) + 1
        half, full = jnp.bfloat16, jnp.float32
        dma = pltpu.SemaphoreType.DMA
        anywhere = pl.BlockSpec(memory_space=pl.ANY)
        vmem = pl.BlockSpec(memory_space=pltpu.VMEM)
        call = pl.pallas_call(
            functools.partial(kernel, (rows, cols, part, depth, width, chunks)),
            out_shape=jax.ShapeDtypeStruct((part, depth), half),
            in_specs=[anywhere, vmem, anywhere, anywhere, anywhere],
            out_specs=vmem,
            scratch_shapes=[
                pltpu.VMEM((rows, part, depth), half),
                pltpu.VMEM((2 * chunks, depth, 2 * width), half),
                pltpu.VMEM((2 * chunks, width, depth), half),
                pltpu.VMEM((2, slots, part, 2 * width), half),
                pltpu.VMEM((2, STAGES, part, 2 * width), half),
                pltpu.VMEM((part, 2 * width), full),
                pltpu.VMEM((2, places, part, width), half),
                pltpu.VMEM((banks, part, depth), full),
                pltpu.VMEM((part, depth), full),
                pltpu.VMEM((rows, part, depth), half),
                pltpu.VMEM((part, depth), half),
                pltpu.VMEM((8, part), full),
                pltpu.VMEM((cols, 8, part), full),
                pltpu.VMEM((8, part), full),
                pltpu.VMEM((rows, 8, part), full),
                pltpu.VMEM((rows, part, 128), full),
                dma,
                dma((2 * chunks,)), dma((2 * chunks,)), dma((2 * chunks,)),
                dma((rows,)), dma((rows,)), dma, dma((rows,)),
                dma((cols,)), dma((cols,)), dma((rows,)), dma((rows,)),
                dma((2, STAGES)), dma((2, slots)), dma((2, places)), dma((2, places)),
            ],
            compiler_params=pltpu.CompilerParams(
                collective_id=0, has_side_effects=True, vmem_limit_bytes=67_043_328),
        )
        return call(tokens, norm_gain.reshape(1, -1), gate_weight, up_weight, down_weight)

    return body


def solution(mesh):
    placed = (P("row", "col"), P("col"), P("col", "row"), P("col", "row"), P("row", "col"))
    return jax.shard_map(
        make_body(mesh.shape["row"], mesh.shape["col"]),
        mesh=mesh, in_specs=placed, out_specs=P("row", "col"), check_vma=False,
    )
```

```python
import functools

import jax
import jax.numpy as jnp
from jax import lax
from jax.experimental import pallas as pl
from jax.experimental.pallas import tpu as pltpu
from jax.sharding import PartitionSpec as P

MESH = pl.DeviceIdType.MESH
LAG_SUM = 2
LAG_HID = 2
STAGES = 4
KEEP = 2
PIECES = 4
AHEAD = 2


def exclusive_or(a, b, bits):
    total = a + b
    for bit in range(bits):
        size = 1 << bit
        total = total - 2 * size * (((a // size) % 2) * ((b // size) % 2))
    return total


def kernel(
    plan, tok, gain, gate_w, up_w, down_w, out,
    xall, wgu, wd, gu_in, gu_out, ybuf, hid, acc, own, rs_in, rs_out,
    sq_out, sq_in, tot_out, tot_in, scale,
    own_sem, wg_sem, wu_sem, wd_sem, ag_send, ag_recv, rs_send, rs_recv,
    sq_send, sq_recv, tot_send, tot_recv, gs_send, gs_recv, hs_send, hs_recv,
):
    rows, cols, part, depth, width, chunks = plan
    hops = cols - 1
    units = rows * chunks
    half = chunks * width
    lag = hops * (LAG_SUM + LAG_HID)
    slots = gu_in.shape[1]
    places = hid.shape[1]
    banks = acc.shape[0]
    bits = rows.bit_length() - 1
    r, p = lax.axis_index("row"), lax.axis_index("col")
    spot = (p, hops - p)
    after = (p + 1, p - 1)
    before = (p - 1, p + 1)
    near = jnp.minimum(spot[0], spot[1])
    far = hops - near

    between = sorted(range(2, rows), key=lambda k: ((k >> 1).bit_count(), k & 1, k))
    order = [0] + between + [1][: rows - 1]

    def mask(i):
        if isinstance(i, int):
            return order[i]
        total = 0
        for at, value in enumerate(order):
            total = total + jnp.where(i == at, value, 0)
        return total

    def partner(i):
        return exclusive_or(r, mask(i), bits)

    def weight_copies(s, j):
        at = s * half + j * width
        c = s * chunks + j
        return (
            pltpu.make_async_copy(gate_w.at[:, pl.ds(at, width)], wgu.at[c, :, pl.ds(0, width)], wg_sem.at[c]),
            pltpu.make_async_copy(up_w.at[:, pl.ds(at, width)], wgu.at[c, :, pl.ds(width, width)], wu_sem.at[c]),
        )

    def down_copy(s, j):
        c = s * chunks + j
        return pltpu.make_async_copy(down_w.at[pl.ds(s * half + j * width, width)], wd.at[c], wd_sem.at[c])

    own_copy = pltpu.make_async_copy(tok, xall.at[0], own_sem)
    own_copy.start()
    for s in (0, 1):
        for one in weight_copies(s, 0):
            one.start()

    barrier = pltpu.get_barrier_semaphore()
    for i in range(1, rows):
        pl.semaphore_signal(barrier, inc=1, device_id=(partner(i), p), device_id_type=MESH)
    for d in range(1, cols):
        pl.semaphore_signal(barrier, inc=1, device_id=(r, (p + d) % cols), device_id_type=MESH)
    pl.semaphore_wait(barrier, rows + cols - 2)

    def spread(i):
        return pltpu.make_async_remote_copy(
            src_ref=tok, dst_ref=xall.at[i], send_sem=ag_send.at[i], recv_sem=ag_recv.at[i],
            device_id=(partner(i), p), device_id_type=MESH)

    for i in range(1, min(AHEAD, rows - 1) + 1):
        spread(i).start()
    for j in range(1, chunks):
        for s in (0, 1):
            for one in weight_copies(s, j):
                one.start()
    for j in range(chunks):
        for s in (0, 1):
            down_copy(s, j).start()

    def square_copy(d):
        return pltpu.make_async_remote_copy(
            src_ref=sq_out, dst_ref=sq_in.at[d], send_sem=sq_send.at[d], recv_sem=sq_recv.at[d],
            device_id=(r, (p + d) % cols), device_id_type=MESH)

    def total_copy(i):
        return pltpu.make_async_remote_copy(
            src_ref=tot_out, dst_ref=tot_in.at[i], send_sem=tot_send.at[i], recv_sem=tot_recv.at[i],
            device_id=(partner(i), p), device_id_type=MESH)

    own_copy.wait()
    squares = jnp.zeros((part, 128), jnp.float32)
    for c in range(depth // 128):
        at = pl.ds(c * 128, 128)
        value = xall[0, :, at].astype(jnp.float32)
        squares = squares + value * value
        xall[0, :, at] = (value * gain[:, at]).astype(jnp.bfloat16)
    sq_out[...] = jnp.broadcast_to(jnp.sum(squares.T, axis=0, keepdims=True), (8, part))
    for d in range(1, cols):
        square_copy(d).start()

    def put_scale(i, total):
        tall = jnp.broadcast_to(total[0:1, :], (128, part)).T
        scale[i] = lax.rsqrt(tall / (depth * cols) + 1e-05)

    def total_squares():
        total = sq_out[...]
        for d in range(1, cols):
            square_copy(d).wait_recv()
            total = total + sq_in[d]
        tot_out[...] = total
        put_scale(0, total)
        for i in range(1, rows):
            total_copy(i).start()

    def sum_copy(s, n):
        stage, slot = lax.rem(n, STAGES), lax.rem(n, slots)
        return pltpu.make_async_remote_copy(
            src_ref=gu_out.at[s, stage], dst_ref=gu_in.at[s, slot],
            send_sem=gs_send.at[s, stage], recv_sem=gs_recv.at[s, slot],
            device_id=(r, after[s]), device_id_type=MESH)

    def hidden_copy(s, m):
        place = lax.rem(m, places)
        return pltpu.make_async_remote_copy(
            src_ref=hid.at[s, place], dst_ref=hid.at[s, place],
            send_sem=hs_send.at[s, place], recv_sem=hs_recv.at[s, place],
            device_id=(r, before[s]), device_id_type=MESH)

    def result_copy(i):
        return pltpu.make_async_remote_copy(
            src_ref=rs_out, dst_ref=rs_in.at[i], send_sem=rs_send, recv_sem=rs_recv.at[i],
            device_id=(partner(i), p), device_id_type=MESH)

    def sums(s, t):
        q = spot[s]
        n = t - LAG_SUM * q
        valid = (n >= 0) & (n < units)

        @pl.when(valid)
        def _():
            i = n // chunks
            j = n - i * chunks

            @pl.when(i == 0)
            def _():
                for one in weight_copies(s, j):
                    one.wait()

            ybuf[...] = jnp.dot(xall[i], wgu[s * chunks + j], preferred_element_type=jnp.float32)

            @pl.when(q > 0)
            def _():
                sum_copy(s, n).wait_recv()
                ybuf[...] += gu_in[s, lax.rem(n, slots)].astype(jnp.float32)

        @pl.when((q < hops) & (n >= STAGES) & (n < units + STAGES))
        def _():
            sum_copy(s, n - STAGES).wait_send()

        @pl.when(valid & (q < hops))
        def _():
            gu_out[s, lax.rem(n, STAGES)] = ybuf[...].astype(jnp.bfloat16)
            sum_copy(s, n).start()

        @pl.when(valid & (q == hops))
        def _():
            factor = scale[n // chunks]
            for c in range(width // 128):
                g = ybuf[:, pl.ds(c * 128, 128)] * factor
                u = ybuf[:, pl.ds(width + c * 128, 128)] * factor
                hid[s, lax.rem(n, places), :, pl.ds(c * 128, 128)] = (jax.nn.silu(g) * u).astype(jnp.bfloat16)
            hidden_copy(s, n).start()

    def hiddens(s, t):
        q = spot[s]
        m = t - lag + LAG_HID * q
        valid = (m >= 0) & (m < units)
        place = lax.rem(jnp.maximum(m, 0), places)

        @pl.when(valid & (q < hops))
        def _():
            hidden_copy(s, m).wait_recv()

        @pl.when(valid & (q < hops) & (q > 0))
        def _():
            hidden_copy(s, m).start()

        @pl.when(valid)
        def _():
            i = m // chunks
            j = m - i * chunks
            bank = lax.rem(i, banks)

            @pl.when(i == 0)
            def _():
                down_copy(s, j).wait()

            leads = (q == far) if s == 0 else ((q == far) & (spot[0] != far))
            fresh = leads & (j == 0)
            wide = depth // PIECES
            for c in range(PIECES):
                at = pl.ds(c * wide, wide)
                value = jnp.dot(hid[s, place], wd[s * chunks + j, :, at], preferred_element_type=jnp.float32)

                @pl.when(fresh)
                def _():
                    acc[bank, :, at] = value

                @pl.when(jnp.logical_not(fresh))
                def _():
                    acc[bank, :, at] += value

        @pl.when((q > 0) & (m >= KEEP) & (m < units + KEEP))
        def _():
            hidden_copy(s, m - KEEP).wait_send()

    def step(t, carry):
        first = t - LAG_SUM * near
        later = first // chunks + AHEAD

        @pl.when((first >= chunks) & (first % chunks == 0) & (later < rows))
        def _():
            spread(later).start()

        @pl.when((first >= chunks) & (first < units) & (first % chunks == 0))
        def _():
            i = first // chunks
            spread(i).wait_recv()
            total_copy(i).wait_recv()
            for c in range(depth // 128):
                at = pl.ds(c * 128, 128)
                xall[i, :, at] = (xall[i, :, at].astype(jnp.float32) * gain[:, at]).astype(jnp.bfloat16)
            put_scale(i, tot_in[i])

        sums(0, t)
        sums(1, t)

        @pl.when(first == 1)
        def _():
            total_squares()

        hiddens(0, t)
        hiddens(1, t)

        last = t - lag + LAG_HID * near

        @pl.when((last >= 0) & (last < units) & (last % chunks == chunks - 1))
        def _():
            i = last // chunks
            bank = lax.rem(i, banks)

            @pl.when(i == 0)
            def _():
                own[...] = acc[bank]

            @pl.when(i >= 2)
            def _():
                result_copy(i - 1).wait_send()

            @pl.when(i > 0)
            def _():
                rs_out[...] = acc[bank].astype(jnp.bfloat16)
                result_copy(i).start()

            @pl.when(i >= 2)
            def _():
                result_copy(i - 1).wait_recv()
                own[...] += rs_in[i - 1].astype(jnp.float32)

        return carry

    lax.fori_loop(0, units + lag + KEEP, step, 0)

    if rows > 1:
        result_copy(rows - 1).wait_send()
        result_copy(rows - 1).wait_recv()
        out[...] = (own[...] + rs_in[rows - 1].astype(jnp.float32)).astype(jnp.bfloat16)
    else:
        out[...] = own[...].astype(jnp.bfloat16)
    for i in range(1, rows):
        spread(i).wait_send()
        total_copy(i).wait_send()
    for d in range(1, cols):
        square_copy(d).wait_send()


def make_body(rows, cols):
    hops = cols - 1
    assert rows & (rows - 1) == 0 and cols > 1

    def body(tokens, norm_gain, gate_weight, up_weight, down_weight):
        part, depth = tokens.shape
        wide = gate_weight.shape[1]
        width = 256 if wide % 512 == 0 else 128
        chunks = wide // (2 * width)
        assert part == 128 and wide % (2 * width) == 0
        lag = hops * (LAG_SUM + LAG_HID)
        slots, places = lag + 2, lag + 2 + KEEP
        banks = -(-LAG_HID * hops // chunks) + 1
        half, full = jnp.bfloat16, jnp.float32
        dma = pltpu.SemaphoreType.DMA
        anywhere = pl.BlockSpec(memory_space=pl.ANY)
        vmem = pl.BlockSpec(memory_space=pltpu.VMEM)
        call = pl.pallas_call(
            functools.partial(kernel, (rows, cols, part, depth, width, chunks)),
            out_shape=jax.ShapeDtypeStruct((part, depth), half),
            in_specs=[anywhere, vmem, anywhere, anywhere, anywhere],
            out_specs=vmem,
            scratch_shapes=[
                pltpu.VMEM((rows, part, depth), half),
                pltpu.VMEM((2 * chunks, depth, 2 * width), half),
                pltpu.VMEM((2 * chunks, width, depth), half),
                pltpu.VMEM((2, slots, part, 2 * width), half),
                pltpu.VMEM((2, STAGES, part, 2 * width), half),
                pltpu.VMEM((part, 2 * width), full),
                pltpu.VMEM((2, places, part, width), half),
                pltpu.VMEM((banks, part, depth), full),
                pltpu.VMEM((part, depth), full),
                pltpu.VMEM((rows, part, depth), half),
                pltpu.VMEM((part, depth), half),
                pltpu.VMEM((8, part), full),
                pltpu.VMEM((cols, 8, part), full),
                pltpu.VMEM((8, part), full),
                pltpu.VMEM((rows, 8, part), full),
                pltpu.VMEM((rows, part, 128), full),
                dma,
                dma((2 * chunks,)), dma((2 * chunks,)), dma((2 * chunks,)),
                dma((rows,)), dma((rows,)), dma, dma((rows,)),
                dma((cols,)), dma((cols,)), dma((rows,)), dma((rows,)),
                dma((2, STAGES)), dma((2, slots)), dma((2, places)), dma((2, places)),
            ],
            compiler_params=pltpu.CompilerParams(
                collective_id=0, has_side_effects=True, vmem_limit_bytes=67_043_328),
        )
        return call(tokens, norm_gain.reshape(1, -1), gate_weight, up_weight, down_weight)

    return body


def solution(mesh):
    placed = (P("row", "col"), P("col"), P("col", "row"), P("col", "row"), P("row", "col"))
    return jax.shard_map(
        make_body(mesh.shape["row"], mesh.shape["col"]),
        mesh=mesh, in_specs=placed, out_specs=P("row", "col"), check_vma=False,
    )
```

```python
import functools

import jax
import jax.numpy as jnp
from jax import lax
from jax.experimental import pallas as pl
from jax.experimental.pallas import tpu as pltpu
from jax.sharding import PartitionSpec as P

MESH = pl.DeviceIdType.MESH
LAG_SUM = (2, 2, 2)
LAG_HID = (2, 2, 2)
SPLIT = 1
SPLIT_HID = 1
SPLIT_OUT = 4
STAGES = 4
KEEP = 2
PIECES = 4
FETCH = 2
AHEAD = 2


def exclusive_or(a, b, bits):
    total = a + b
    for bit in range(bits):
        size = 1 << bit
        total = total - 2 * size * (((a // size) % 2) * ((b // size) % 2))
    return total


def lags(hops):
    there = sum(LAG_SUM[h % len(LAG_SUM)] for h in range(hops))
    return there, there + sum(LAG_HID[h % len(LAG_HID)] for h in range(hops))


def kernel(
    plan, tok, gain, gate_w, up_w, down_w, out,
    xall, wgu, wd, gu_in, gu_out, ybuf, hid, acc, own, rs_in, rs_out,
    sq_out, sq_in, tot_out, tot_in, scale,
    own_sem, wg_sem, wu_sem, wd_sem, ag_send, ag_recv, rs_send, rs_recv,
    sq_send, sq_recv, tot_send, tot_recv, gs_send, gs_recv, hs_send, hs_recv,
):
    rows, cols, part, depth, width, chunks = plan
    hops = cols - 1
    units = rows * chunks
    half = chunks * width
    there, lag = lags(hops)
    slots = gu_in.shape[1]
    places = hid.shape[1]
    banks = acc.shape[0]
    bits = rows.bit_length() - 1
    r, p = lax.axis_index("row"), lax.axis_index("col")
    spot = (p, hops - p)
    after = (p + 1, p - 1)
    before = (p - 1, p + 1)
    near = jnp.minimum(spot[0], spot[1])
    far = hops - near

    def sum_lag(q):
        return sum(jnp.where(q > h, LAG_SUM[h % len(LAG_SUM)], 0) for h in range(hops))

    def hidden_lag(q):
        return there + sum(jnp.where(hops - q > h, LAG_HID[h % len(LAG_HID)], 0) for h in range(hops))

    def cut(k, pieces):
        return pl.ds(k * (part // pieces), part // pieces)

    between = sorted(range(2, rows), key=lambda k: ((k >> 1).bit_count(), k & 1, k))
    order = [0] + between + [1][: rows - 1]

    def mask(i):
        if isinstance(i, int):
            return order[i]
        total = 0
        for at, value in enumerate(order):
            total = total + jnp.where(i == at, value, 0)
        return total

    def partner(i):
        return exclusive_or(r, mask(i), bits)

    def weight_copies(s, j):
        at = pl.multiple_of(s * half + j * width, 128)
        c = s * chunks + j
        return (
            pltpu.make_async_copy(gate_w.at[:, pl.ds(at, width)], wgu.at[c, :, pl.ds(0, width)], wg_sem.at[c]),
            pltpu.make_async_copy(up_w.at[:, pl.ds(at, width)], wgu.at[c, :, pl.ds(width, width)], wu_sem.at[c]),
        )

    def down_copy(s, j):
        c = s * chunks + j
        return pltpu.make_async_copy(down_w.at[pl.ds(pl.multiple_of(s * half + j * width, 128), width)], wd.at[c], wd_sem.at[c])

    own_copy = pltpu.make_async_copy(tok, xall.at[0], own_sem)
    own_copy.start()
    for s in (0, 1):
        for one in weight_copies(s, 0):
            one.start()

    barrier = pltpu.get_barrier_semaphore()
    for i in range(1, rows):
        pl.semaphore_signal(barrier, inc=1, device_id=(partner(i), p), device_id_type=MESH)
    for d in range(1, cols):
        pl.semaphore_signal(barrier, inc=1, device_id=(r, (p + d) % cols), device_id_type=MESH)
    pl.semaphore_wait(barrier, rows + cols - 2)

    def spread(i):
        return pltpu.make_async_remote_copy(
            src_ref=tok, dst_ref=xall.at[i], send_sem=ag_send.at[i], recv_sem=ag_recv.at[i],
            device_id=(partner(i), p), device_id_type=MESH)

    for i in range(1, min(AHEAD, rows - 1) + 1):
        spread(i).start()
    for j in range(FETCH):
        for s in (0, 1):
            if j > 0:
                for one in weight_copies(s, j):
                    one.start()
            down_copy(s, j).start()

    def square_copy(d):
        return pltpu.make_async_remote_copy(
            src_ref=sq_out, dst_ref=sq_in.at[d], send_sem=sq_send.at[d], recv_sem=sq_recv.at[d],
            device_id=(r, (p + d) % cols), device_id_type=MESH)

    def total_copy(i):
        return pltpu.make_async_remote_copy(
            src_ref=tot_out, dst_ref=tot_in.at[i], send_sem=tot_send.at[i], recv_sem=tot_recv.at[i],
            device_id=(partner(i), p), device_id_type=MESH)

    own_copy.wait()
    for c in range(depth // 128):
        at = pl.ds(c * 128, 128)
        value = xall[0, :, at].astype(jnp.float32)
        ybuf[0, :, 0:128] = value * value if c == 0 else ybuf[0, :, 0:128] + value * value
        xall[0, :, at] = (value * gain[:, at]).astype(jnp.bfloat16)
    sq_out[...] = jnp.broadcast_to(jnp.sum(ybuf[0, :, 0:128].T, axis=0, keepdims=True), (8, part))
    for d in range(1, cols):
        square_copy(d).start()

    def put_scale(i, total):
        tall = jnp.broadcast_to(total[0:1, :], (128, part)).T
        scale[i] = lax.rsqrt(tall / (depth * cols) + 1e-05)

    def total_squares():
        total = sq_out[...]
        for d in range(1, cols):
            square_copy(d).wait_recv()
            total = total + sq_in[d]
        tot_out[...] = total
        put_scale(0, total)
        for i in range(1, rows):
            total_copy(i).start()

    def sum_copy(s, n, k):
        stage, slot = lax.rem(n, STAGES), lax.rem(n, slots)
        at = cut(k, SPLIT)
        return pltpu.make_async_remote_copy(
            src_ref=gu_out.at[s, stage, at], dst_ref=gu_in.at[s, slot, at],
            send_sem=gs_send.at[s, stage, k], recv_sem=gs_recv.at[s, slot, k],
            device_id=(r, after[s]), device_id_type=MESH)

    def hidden_copy(s, m, k):
        place = lax.rem(m, places)
        at = cut(k, SPLIT_HID)
        return pltpu.make_async_remote_copy(
            src_ref=hid.at[s, place, at], dst_ref=hid.at[s, place, at],
            send_sem=hs_send.at[s, place, k], recv_sem=hs_recv.at[s, place, k],
            device_id=(r, before[s]), device_id_type=MESH)

    def result_copy(i, k):
        at = cut(k, SPLIT_OUT)
        return pltpu.make_async_remote_copy(
            src_ref=rs_out.at[at], dst_ref=rs_in.at[i - 1, at],
            send_sem=rs_send.at[k], recv_sem=rs_recv.at[i - 1, k],
            device_id=(partner(i), p), device_id_type=MESH)

    def multiply(s, t):
        n = t - sum_lag(spot[s])

        @pl.when((n >= 0) & (n < units))
        def _():
            i = n // chunks
            j = n - i * chunks

            @pl.when(i == 0)
            def _():
                for one in weight_copies(s, j):
                    one.wait()

                @pl.when(j < chunks - FETCH)
                def _():
                    for one in weight_copies(s, j + FETCH):
                        one.start()
                    down_copy(s, j + FETCH).start()

            ybuf[s] = jnp.dot(xall[i], wgu[s * chunks + j], preferred_element_type=jnp.float32)

    def sums(s, t):
        q = spot[s]
        n = t - sum_lag(q)
        valid = (n >= 0) & (n < units)

        @pl.when((q < hops) & (n >= STAGES) & (n < units + STAGES))
        def _():
            for k in range(SPLIT):
                sum_copy(s, n - STAGES, k).wait_send()

        @pl.when(valid & (q == 0))
        def _():
            for k in range(SPLIT):
                at = cut(k, SPLIT)
                gu_out[s, lax.rem(n, STAGES), at] = ybuf[s, at].astype(jnp.bfloat16)
                sum_copy(s, n, k).start()

        @pl.when(valid & (q > 0) & (q < hops))
        def _():
            for k in range(SPLIT):
                at = cut(k, SPLIT)
                sum_copy(s, n, k).wait_recv()
                total = ybuf[s, at] + gu_in[s, lax.rem(n, slots), at].astype(jnp.float32)
                gu_out[s, lax.rem(n, STAGES), at] = total.astype(jnp.bfloat16)
                sum_copy(s, n, k).start()

        @pl.when(valid & (q == hops))
        def _():
            i = n // chunks
            every = SPLIT // SPLIT_HID
            for k in range(SPLIT):
                at = cut(k, SPLIT)
                sum_copy(s, n, k).wait_recv()
                factor = scale[i, at]
                for c in range(width // 128):
                    left, right = pl.ds(c * 128, 128), pl.ds(width + c * 128, 128)
                    g = (ybuf[s, at, left] + gu_in[s, lax.rem(n, slots), at, left].astype(jnp.float32)) * factor
                    u = (ybuf[s, at, right] + gu_in[s, lax.rem(n, slots), at, right].astype(jnp.float32)) * factor
                    hid[s, lax.rem(n, places), at, left] = (jax.nn.silu(g) * u).astype(jnp.bfloat16)
                if k % every == every - 1:
                    hidden_copy(s, n, k // every).start()

    def hiddens(s, t):
        q = spot[s]
        m = t - hidden_lag(q)
        valid = (m >= 0) & (m < units)

        @pl.when(valid & (q == 0))
        def _():
            for k in range(SPLIT_HID):
                hidden_copy(s, m, k).wait_recv()

        @pl.when(valid & (q < hops) & (q > 0))
        def _():
            for k in range(SPLIT_HID):
                hidden_copy(s, m, k).wait_recv()
                hidden_copy(s, m, k).start()

    def project(s, t):
        q = spot[s]
        m = t - hidden_lag(q)
        valid = (m >= 0) & (m < units)
        place = lax.rem(jnp.maximum(m, 0), places)

        @pl.when(valid)
        def _():
            i = m // chunks
            j = m - i * chunks
            bank = lax.rem(i, banks)

            @pl.when(i == 0)
            def _():
                down_copy(s, j).wait()

            leads = (q == far) if s == 0 else ((q == far) & (spot[0] != far))
            fresh = leads & (j == 0)
            wide = depth // PIECES
            for c in range(PIECES):
                at = pl.ds(c * wide, wide)
                value = jnp.dot(hid[s, place], wd[s * chunks + j, :, at], preferred_element_type=jnp.float32)

                @pl.when(fresh)
                def _():
                    acc[bank, :, at] = value

                @pl.when(jnp.logical_not(fresh))
                def _():
                    acc[bank, :, at] += value

        @pl.when((q > 0) & (m >= KEEP) & (m < units + KEEP))
        def _():
            for k in range(SPLIT_HID):
                hidden_copy(s, m - KEEP, k).wait_send()

    def prepare(t):
        first = t - sum_lag(near)
        later = first // chunks + AHEAD

        @pl.when((first >= chunks) & (first % chunks == 0) & (later < rows))
        def _():
            spread(later).start()

        @pl.when((first >= chunks) & (first < units) & (first % chunks == 0))
        def _():
            i = first // chunks
            spread(i).wait_recv()
            total_copy(i).wait_recv()
            for c in range(depth // 128):
                at = pl.ds(c * 128, 128)
                xall[i, :, at] = (xall[i, :, at].astype(jnp.float32) * gain[:, at]).astype(jnp.bfloat16)
            put_scale(i, tot_in[i])

    def step(t, carry):
        sums(0, t)
        sums(1, t)
        hiddens(0, t)
        hiddens(1, t)

        @pl.when(t - sum_lag(near) == 1)
        def _():
            total_squares()

        prepare(t + 1)
        multiply(0, t + 1)
        multiply(1, t + 1)
        project(0, t)
        project(1, t)

        last = t - hidden_lag(near)

        @pl.when((last >= 0) & (last < units) & (last % chunks == chunks - 1))
        def _():
            i = last // chunks
            bank = lax.rem(i, banks)

            @pl.when(i == 0)
            def _():
                own[...] = acc[bank]

            @pl.when(i >= 2)
            def _():
                for k in range(SPLIT_OUT):
                    result_copy(i - 1, k).wait_send()

            @pl.when(i > 0)
            def _():
                for k in range(SPLIT_OUT):
                    at = cut(k, SPLIT_OUT)
                    rs_out[at] = acc[bank, at].astype(jnp.bfloat16)
                    result_copy(i, k).start()

            @pl.when(i >= 2)
            def _():
                for k in range(SPLIT_OUT):
                    at = cut(k, SPLIT_OUT)
                    result_copy(i - 1, k).wait_recv()
                    own[at] += rs_in[i - 2, at].astype(jnp.float32)

        return carry

    multiply(0, 0)
    multiply(1, 0)
    lax.fori_loop(0, units + lag + KEEP, step, 0)

    for k in range(SPLIT_OUT):
        at = cut(k, SPLIT_OUT)
        result_copy(rows - 1, k).wait_recv()
        out[at] = (own[at] + rs_in[rows - 2, at].astype(jnp.float32)).astype(jnp.bfloat16)
    for k in range(SPLIT_OUT):
        result_copy(rows - 1, k).wait_send()
    for i in range(1, rows):
        spread(i).wait_send()
        total_copy(i).wait_send()
    for d in range(1, cols):
        square_copy(d).wait_send()


def make_body(rows, cols):
    hops = cols - 1
    assert rows & (rows - 1) == 0 and min(rows, cols) > 1

    def body(tokens, norm_gain, gate_weight, up_weight, down_weight):
        part, depth = tokens.shape
        wide = gate_weight.shape[1]
        width = 256 if wide % 512 == 0 else 128
        chunks = wide // (2 * width)
        assert part == 128 and wide % (2 * width) == 0 and chunks >= FETCH
        there, lag = lags(hops)
        slots, places = lag + 2, lag + 2 + KEEP
        banks = -(-(lag - there) // chunks) + 1
        half, full = jnp.bfloat16, jnp.float32
        dma = pltpu.SemaphoreType.DMA
        anywhere = pl.BlockSpec(memory_space=pl.ANY)
        vmem = pl.BlockSpec(memory_space=pltpu.VMEM)
        call = pl.pallas_call(
            functools.partial(kernel, (rows, cols, part, depth, width, chunks)),
            out_shape=pltpu.VMEM((part, depth), half),
            in_specs=[anywhere, vmem, anywhere, anywhere, anywhere],
            out_specs=vmem,
            scratch_shapes=[
                pltpu.VMEM((rows, part, depth), half),
                pltpu.VMEM((2 * chunks, depth, 2 * width), half),
                pltpu.VMEM((2 * chunks, width, depth), half),
                pltpu.VMEM((2, slots, part, 2 * width), half),
                pltpu.VMEM((2, STAGES, part, 2 * width), half),
                pltpu.VMEM((2, part, 2 * width), full),
                pltpu.VMEM((2, places, part, width), half),
                pltpu.VMEM((banks, part, depth), full),
                pltpu.VMEM((part, depth), full),
                pltpu.VMEM((rows - 1, part, depth), half),
                pltpu.VMEM((part, depth), half),
                pltpu.VMEM((8, part), full),
                pltpu.VMEM((cols, 8, part), full),
                pltpu.VMEM((8, part), full),
                pltpu.VMEM((rows, 8, part), full),
                pltpu.VMEM((rows, part, 128), full),
                dma,
                dma((2 * chunks,)), dma((2 * chunks,)), dma((2 * chunks,)),
                dma((rows,)), dma((rows,)), dma((SPLIT_OUT,)), dma((rows - 1, SPLIT_OUT)),
                dma((cols,)), dma((cols,)), dma((rows,)), dma((rows,)),
                dma((2, STAGES, SPLIT)), dma((2, slots, SPLIT)), dma((2, places, SPLIT_HID)), dma((2, places, SPLIT_HID)),
            ],
            compiler_params=pltpu.CompilerParams(
                collective_id=0, has_side_effects=True, vmem_limit_bytes=66_000_000),
        )
        return call(tokens, norm_gain.reshape(1, -1), gate_weight, up_weight, down_weight)

    return body


def solution(mesh):
    placed = (P("row", "col"), P("col"), P("col", "row"), P("col", "row"), P("row", "col"))
    return jax.shard_map(
        make_body(mesh.shape["row"], mesh.shape["col"]),
        mesh=mesh, in_specs=placed, out_specs=P("row", "col"), check_vma=False,
    )
```
